32 devices in a mesh: dp: 8 (over y, x, core), expert: 4 (over z).
Axes of the slice: x: 2, y: 2, z: 4, core: 2. Of those that a mesh axis runs over, the one named last changes fastest.
Arguments:
- tokens: bfloat16 [512, 2048], P('expert', 'dp'), may hold values from -6 to 6
- routes: int32 [512, 2], P('expert'), may hold values from 0 to 3, all different within a row
- dt_raw: float32 [512, 32], P('expert', 'dp'), may hold values from -5 to 5
- b_proj: float32 [512, 16], P('expert'), may hold values from -1.8 to 1.8
- c_proj: float32 [512, 16], P('expert'), may hold values from -1.8 to 1.8
- decay_rate: float32 [32], P('dp'), may hold values from 0.002 to 0.2
- skip_gain: float32 [32], P('dp'), may hold values from 0.5 to 1.5
- router_weight: float32 [2048, 4], P('dp'), may hold values from -0.125 to 0.125
- gate_weight: bfloat16 [4, 2048, 7168], P('expert', None, 'dp'), may hold values from -0.125 to 0.125
- up_weight: bfloat16 [4, 2048, 7168], P('expert', None, 'dp'), may hold values from -0.125 to 0.125
- down_weight: bfloat16 [4, 7168, 2048], P('expert', 'dp'), may hold values from -0.0625 to 0.0625
- out_grad: bfloat16 [512, 2048], P('expert', 'dp'), may hold values from -6 to 6
Outputs:
- block_out: bfloat16 [512, 2048], P('expert', 'dp')
- token_grad: bfloat16 [512, 2048], P('expert', 'dp')
- gate_grad: bfloat16 [4, 2048, 7168], P('expert', None, 'dp')
- up_grad: bfloat16 [4, 2048, 7168], P('expert', None, 'dp')
- down_grad: bfloat16 [4, 7168, 2048], P('expert', 'dp')
- router_grad: float32 [2048, 4], P('dp')
- rate_grad: float32 [32], P('dp')
- skip_grad: float32 [32], P('dp')
The draws below stay inside these ranges and needn't reach their ends.
Inputs may be any that keep to these rules, and one draw needn't show every extreme that they name: `routes`: each token names two different experts.
All inputs are finite; a program needn't handle non-finite values.
Results may differ from the reference program's by a relative error of at most 0.02.
Values may be sent and summed in bfloat16 or wider, within the bound.
A program may use at most 64 MiB of HBM per device.

```python
import math
import jax
import jax.numpy as jnp
from jax import lax

D = 2048
FF = 7168
HEAD_DIM = 64
STATE = 16
TOK_DEV = 128
CAP = 80
HEADS = 32
EXPERTS = 4
LENGTH = 512
N_DP = 8
N_EXPERT = 4


def shard_levels(rng, dims, cuts, least, largest):
    level, own = 1.0, jax.random.fold_in(rng, 6)
    for position, shards_of in cuts:
        draws = jnp.exp(jax.random.uniform(jax.random.fold_in(own, position), (shards_of,), jnp.float32, least / len(cuts), largest / len(cuts)))
        level = level * jnp.repeat(draws, dims[position] // shards_of).reshape([-1 if axis == position else 1 for axis in range(len(dims))])
    return level


def different_ones(rng, rows, amount, top, lift):
    order = jax.random.permutation(jax.random.fold_in(rng, 1), amount)
    favour = order
    for power in range(3):
        favour = favour * favour // amount
    favour = favour * lift // amount
    lots = jax.random.randint(jax.random.fold_in(rng, 2), (rows, amount), 0, 4096) + favour
    fixed_rows = jax.random.permutation(jax.random.fold_in(rng, 3), rows)[jnp.arange(amount) % rows]
    lots = jnp.where(jnp.arange(rows)[:, None] == fixed_rows[None, :], 1 << 14, lots)
    priority = lots * amount + jnp.arange(amount)
    return lax.top_k(priority.astype(jnp.int32), top)[1].astype(jnp.int32)


def normal_values(stream_key, dims, scale, bound, cuts=(), kind=jnp.bfloat16):
    loudness = shard_levels(stream_key, dims, cuts, -0.22, 0.18) if cuts else 1.0
    drawn = jax.random.normal(stream_key, dims, jnp.float32) * scale * loudness
    return jnp.minimum(jnp.maximum(drawn, -bound), bound).astype(kind)


def setup_inputs(seed: int = 0) -> dict:
    splits = jax.random.split(jax.random.key(seed), 13)
    tokens = normal_values(splits[0], (LENGTH, D), 1.0, 6.0, ((0, 4), (1, 8)))
    routes = different_ones(splits[1], LENGTH, EXPERTS, 2, 8192)
    dt_raw = normal_values(splits[2], (LENGTH, HEADS), 1.0, 5.0, ((0, 4), (1, 8)), jnp.float32)
    b_proj = normal_values(splits[3], (LENGTH, STATE), 0.3, 1.8, ((0, 4),), jnp.float32)
    c_proj = normal_values(splits[4], (LENGTH, STATE), 0.3, 1.8, ((0, 4),), jnp.float32)
    decay_rate = jnp.clip(jnp.exp(math.log(0.2) - 4.6051702 * jax.random.uniform(splits[5], (HEADS,), jnp.float32) ** shard_levels(splits[5], (HEADS,), ((0, 8),), -0.2, 0.2)), 0.002, 0.2)
    skip_gain = jnp.clip(0.5 + 1.0 * jax.random.uniform(splits[6], (HEADS,), jnp.float32) ** shard_levels(splits[6], (HEADS,), ((0, 8),), -0.2, 0.2), 0.5, 1.5)
    router_weight = normal_values(splits[7], (D, EXPERTS), D ** -0.5, 0.125, ((0, 8),), jnp.float32)
    gate_weight = normal_values(splits[8], (EXPERTS, D, FF), D ** -0.5, 0.125, ((0, 4), (2, 8)))
    up_weight = normal_values(splits[9], (EXPERTS, D, FF), D ** -0.5, 0.125, ((0, 4), (2, 8)))
    down_weight = normal_values(splits[10], (EXPERTS, FF, D), FF ** -0.5, 0.0625, ((0, 4), (1, 8)))
    out_grad = normal_values(splits[11], (LENGTH, D), 1.0, 6.0, ((0, 4), (1, 8)))
    return {"tokens": tokens, "routes": routes, "dt_raw": dt_raw, "b_proj": b_proj, "c_proj": c_proj, "decay_rate": decay_rate, "skip_gain": skip_gain, "router_weight": router_weight, "gate_weight": gate_weight, "up_weight": up_weight, "down_weight": down_weight, "out_grad": out_grad}


EPSILON = 1e-06
HIGHEST = lax.Precision.HIGHEST

def rms_norm(values):
    return values * lax.rsqrt(lax.optimization_barrier(jnp.mean(values * values, axis=-1, keepdims=True)) + EPSILON)

def end_parts(normed, b_rows, dt_rows, decay_rate):
    steps_total = normed.shape[0]
    head_count = decay_rate.shape[0]
    step_size = jax.nn.softplus(dt_rows)
    running = jnp.cumsum(-step_size * decay_rate[None, :], axis=0)
    tail_weight = jnp.exp(running[-1][None, :] - running) * step_size
    head_rows = normed.reshape(steps_total, head_count, -1)
    local_state = jnp.einsum('sh,shp,sn->hpn', tail_weight, head_rows, b_rows, precision=HIGHEST)
    return (jnp.exp(running[-1]), local_state.reshape(head_count, -1))

def ssd_piece(normed, b_rows, c_rows, dt_rows, decay_rate, skip_gain, state_start):
    steps_total = normed.shape[0]
    head_count = decay_rate.shape[0]
    state_width = b_rows.shape[1]
    step_size = jax.nn.softplus(dt_rows)
    running = jnp.cumsum(-step_size * decay_rate[None, :], axis=0)
    positions = jnp.arange(steps_total, dtype=jnp.int32)
    causal = (positions[:, None] >= positions[None, :])[:, :, None]
    spread = jnp.where(causal, running[:, None, :] - running[None, :, :], 0.0)
    decay_table = jnp.where(causal, jnp.exp(spread), 0.0)
    pairing = jnp.dot(c_rows, b_rows.T, precision=HIGHEST)
    mixing = decay_table * pairing[:, :, None] * step_size[None, :, :]
    head_rows = normed.reshape(steps_total, head_count, -1)
    state_three = state_start.reshape(head_count, -1, state_width)
    mixed = jnp.einsum('tsh,shp->thp', mixing, head_rows, precision=HIGHEST)
    mixed = mixed + jnp.einsum('tn,th,hpn->thp', c_rows, jnp.exp(running), state_three, precision=HIGHEST)
    mixed = mixed + skip_gain[None, :, None] * head_rows
    decay_total, local_state = end_parts(normed, b_rows, dt_rows, decay_rate)
    state_end = decay_total[:, None] * state_start + local_state
    return (mixed.reshape(steps_total, -1), state_end)

def dispatch_table(choice_ids, expert_count, capacity):
    flat_ids = choice_ids.reshape(-1)
    row_total = flat_ids.shape[0]
    expert_hot = (flat_ids[:, None] == jnp.arange(expert_count, dtype=jnp.int32)[None, :]).astype(jnp.float32)
    positions = jnp.arange(row_total, dtype=jnp.int32)
    lower = (positions[:, None] > positions[None, :]).astype(jnp.float32)
    earlier = jnp.dot(lower, expert_hot, precision=HIGHEST)
    slot_index = lax.optimization_barrier(jnp.sum(earlier * expert_hot, axis=1))
    target = flat_ids.astype(jnp.float32) * capacity + slot_index
    target = jnp.where(slot_index < capacity, target, -1.0)
    slot_ids = jnp.arange(expert_count * capacity, dtype=jnp.int32).astype(jnp.float32)
    return (slot_ids[:, None] == target[None, :]).astype(jnp.float32)

def block_sum(parts):
    rounded = lax.optimization_barrier(parts.astype(jnp.bfloat16))
    return lax.optimization_barrier(jnp.sum(rounded.astype(jnp.float32), axis=1)).astype(jnp.bfloat16)

def reference(tokens, routes, dt_raw, b_proj, c_proj, decay_rate, skip_gain, router_weight, gate_weight, up_weight, down_weight, out_grad):
    blocks = N_EXPERT
    unit_size = FF // N_DP
    inputs = tokens.astype(jnp.float32)

    def mixer_all(inputs_in, rate_in, skip_in):
        normed = rms_norm(inputs_in).reshape(blocks, TOK_DEV, D)

        def one_block(state, pieces):
            normed_rows, b_rows, c_rows, dt_rows = pieces
            mixed_rows, state_end = ssd_piece(normed_rows, b_rows, c_rows, dt_rows, rate_in, skip_in, state)
            return (state_end, mixed_rows)
        zero_state = jnp.zeros((HEADS, HEAD_DIM * STATE), jnp.float32)
        final_state, mixed_all = lax.scan(one_block, zero_state, (normed, b_proj.reshape(blocks, TOK_DEV, STATE), c_proj.reshape(blocks, TOK_DEV, STATE), dt_raw.reshape(blocks, TOK_DEV, HEADS)))
        return mixed_all.reshape(LENGTH, D)
    mixed, mixer_pull = jax.vjp(mixer_all, inputs, decay_rate, skip_gain)
    resid = (inputs + mixed).astype(jnp.bfloat16)
    resid_f = resid.astype(jnp.float32).reshape(blocks, TOK_DEV, D)
    pre_moe, norm_pull = jax.vjp(rms_norm, resid_f)
    moe_in = pre_moe.astype(jnp.bfloat16)
    moe_f = moe_in.astype(jnp.float32)
    choice_ids = routes.reshape(blocks, TOK_DEV, 2)
    logits = jnp.einsum('btd,de->bte', moe_f, router_weight, precision=HIGHEST)
    expert_ids = jnp.arange(EXPERTS, dtype=jnp.int32)
    first_hot = (choice_ids[:, :, 0:1] == expert_ids).astype(jnp.float32)
    second_hot = (choice_ids[:, :, 1:2] == expert_ids).astype(jnp.float32)
    logit_gap = lax.optimization_barrier(jnp.sum(logits * (first_hot - second_hot), axis=2))
    first_weight = jax.nn.sigmoid(logit_gap)
    second_weight = jax.nn.sigmoid(-logit_gap)
    tables = jax.vmap(lambda ids_block: dispatch_table(ids_block, EXPERTS, CAP))(choice_ids)
    doubled = jnp.repeat(moe_f, 2, axis=1)
    send_rows = jnp.einsum('bsp,bpd->bsd', tables, doubled, precision=HIGHEST).astype(jnp.bfloat16)

    def to_experts(rows):
        shaped = rows.reshape(N_EXPERT, EXPERTS, CAP, D)
        return shaped.transpose(1, 0, 2, 3).reshape(EXPERTS, blocks * CAP, D)

    def from_experts(rows):
        shaped = rows.reshape(EXPERTS, N_EXPERT, CAP, D)
        return shaped.transpose(1, 0, 2, 3).reshape(blocks, EXPERTS * CAP, D)
    expert_rows = to_experts(send_rows)

    def expert_forward(pieces):
        rows, gate_w, up_w, down_w = pieces
        gate_pre = jnp.dot(rows, gate_w, preferred_element_type=jnp.float32)
        up_pre = jnp.dot(rows, up_w, preferred_element_type=jnp.float32)
        hidden = (jax.nn.silu(gate_pre) * up_pre).astype(jnp.bfloat16)
        parts = jnp.einsum('rbf,bfd->rbd', hidden.astype(jnp.float32).reshape(-1, N_DP, unit_size), down_w.astype(jnp.float32).reshape(N_DP, unit_size, D), precision=HIGHEST)
        return block_sum(parts)
    expert_out = lax.map(expert_forward, (expert_rows, gate_weight, up_weight, down_weight))
    back_rows = from_experts(expert_out).astype(jnp.float32)
    per_slot = jnp.einsum('bsp,bsd->bpd', tables, back_rows, precision=HIGHEST).reshape(blocks, TOK_DEV, 2, D)
    moe_sum = first_weight[:, :, None] * per_slot[:, :, 0] + second_weight[:, :, None] * per_slot[:, :, 1]
    block_out = (resid_f + moe_sum).astype(jnp.bfloat16).reshape(LENGTH, D)
    upstream = out_grad.astype(jnp.float32).reshape(blocks, TOK_DEV, D)
    first_back = lax.optimization_barrier(jnp.sum(upstream * per_slot[:, :, 0], axis=2))
    second_back = lax.optimization_barrier(jnp.sum(upstream * per_slot[:, :, 1], axis=2))
    slot_grad = jnp.stack([first_weight[:, :, None] * upstream, second_weight[:, :, None] * upstream], axis=2)
    slot_grad = slot_grad.reshape(blocks, 2 * TOK_DEV, D).astype(jnp.bfloat16)
    grad_send = jnp.einsum('bsp,bpd->bsd', tables, slot_grad.astype(jnp.float32), precision=HIGHEST).astype(jnp.bfloat16)
    grad_rows_all = to_experts(grad_send)

    def expert_backward(pieces):
        rows, grad_rows, gate_w, up_w, down_w = pieces
        gate_pre = jnp.dot(rows, gate_w, preferred_element_type=jnp.float32)
        up_pre = jnp.dot(rows, up_w, preferred_element_type=jnp.float32)
        hidden = (jax.nn.silu(gate_pre) * up_pre).astype(jnp.bfloat16)
        unit_grad = lax.dot_general(grad_rows, down_w, (((1,), (1,)), ((), ())), preferred_element_type=jnp.float32)
        sigma = jax.nn.sigmoid(gate_pre)
        gate_back = (unit_grad * up_pre * sigma * (1.0 + gate_pre * (1.0 - sigma))).astype(jnp.bfloat16)
        up_back = (unit_grad * jax.nn.silu(gate_pre)).astype(jnp.bfloat16)
        down_part = lax.dot_general(hidden, grad_rows, (((0,), (0,)), ((), ())), preferred_element_type=jnp.float32)
        gate_part = lax.dot_general(rows, gate_back, (((0,), (0,)), ((), ())), preferred_element_type=jnp.float32)
        up_part = lax.dot_general(rows, up_back, (((0,), (0,)), ((), ())), preferred_element_type=jnp.float32)
        parts = jnp.einsum('rbf,dbf->rbd', gate_back.astype(jnp.float32).reshape(-1, N_DP, unit_size), gate_w.astype(jnp.float32).reshape(D, N_DP, unit_size), precision=HIGHEST)
        parts = parts + jnp.einsum('rbf,dbf->rbd', up_back.astype(jnp.float32).reshape(-1, N_DP, unit_size), up_w.astype(jnp.float32).reshape(D, N_DP, unit_size), precision=HIGHEST)
        return (block_sum(parts), gate_part.astype(jnp.bfloat16), up_part.astype(jnp.bfloat16), down_part.astype(jnp.bfloat16))
    input_back, gate_grad, up_grad, down_grad = lax.map(expert_backward, (expert_rows, grad_rows_all, gate_weight, up_weight, down_weight))
    returned = from_experts(input_back).astype(jnp.float32)
    slot_back = jnp.einsum('bsp,bsd->bpd', tables, returned, precision=HIGHEST).reshape(blocks, TOK_DEV, 2, D)
    moe_grad = slot_back[:, :, 0] + slot_back[:, :, 1]
    gap_grad = first_weight * second_weight * (first_back - second_back)
    logit_grad = gap_grad[:, :, None] * (first_hot - second_hot)
    moe_in_grad = moe_grad + jnp.einsum('bte,de->btd', logit_grad, router_weight, precision=HIGHEST)
    router_grad = jnp.einsum('btd,bte->de', moe_f, logit_grad, precision=HIGHEST)
    resid_grad = upstream + norm_pull(moe_in_grad)[0]
    resid_grad = resid_grad.reshape(LENGTH, D)
    mixer_input_grad, rate_grad, skip_grad = mixer_pull(resid_grad)
    token_grad = (resid_grad + mixer_input_grad).astype(jnp.bfloat16)
    return (block_out, token_grad, gate_grad, up_grad, down_grad, router_grad, rate_grad, skip_grad)
```

```python
import functools
import jax
import jax.numpy as jnp
from jax import lax
from jax.experimental import pallas as pl
from jax.experimental.pallas import tpu as pltpu
from jax.sharding import PartitionSpec as P


EPSILON = 1e-06
HIGHEST = lax.Precision.HIGHEST
MESH = pl.DeviceIdType.MESH


def loop(count, step):
    def run(i, carry):
        step(i)
        return carry

    lax.fori_loop(0, count, run, 0)


def greet(axes):
    barrier = pltpu.get_barrier_semaphore()
    total = 0
    for axis in axes:
        peers, place = (lax.axis_size(axis), lax.axis_index(axis))
        total += peers - 1

        def signal(k):
            pl.semaphore_signal(
                barrier, 1, device_id={axis: lax.rem(place + k + 1, peers)}, device_id_type=MESH
            )

        loop(peers - 1, signal)
    pl.semaphore_wait(barrier, total)


def swap_kernel(plan, *refs):
    amount = len(plan)
    ins, outs = (refs[:amount], refs[amount : 2 * amount])
    gathered = refs[2 * amount : 3 * amount]
    sends, recvs = (refs[3 * amount : 4 * amount], refs[4 * amount : 5 * amount])
    greet(sorted({axis for axis, _ in plan}))

    def copy_of(item, k):
        axis = plan[item][0]
        peers, place = (lax.axis_size(axis), lax.axis_index(axis))
        return pltpu.make_async_remote_copy(
            src_ref=ins[item],
            dst_ref=gathered[item].at[place],
            send_sem=sends[item].at[k],
            recv_sem=recvs[item].at[k],
            device_id={axis: lax.rem(place + k + 1, peers)},
            device_id_type=MESH,
        )

    for item, (axis, _) in enumerate(plan):
        loop(lax.axis_size(axis) - 1, lambda k: copy_of(item, k).start())
        gathered[item][lax.axis_index(axis)] = ins[item][...]
    for item, (axis, reduce) in enumerate(plan):
        peers, place = (lax.axis_size(axis), lax.axis_index(axis))

        def arrive(k):
            pltpu.make_async_remote_copy(
                src_ref=ins[item],
                dst_ref=gathered[item].at[lax.rem(place + peers - k - 1, peers)],
                send_sem=sends[item].at[k],
                recv_sem=recvs[item].at[k],
                device_id={axis: lax.rem(place + k + 1, peers)},
                device_id_type=MESH,
            ).wait()

        loop(peers - 1, arrive)
        if reduce:
            outs[item][...] = jnp.sum(gathered[item][...], axis=0)
        else:
            outs[item][...] = gathered[item][...]


def swap(name, number, *items):
    plan = tuple((axis, reduce) for _, axis, reduce in items)
    arrays = [array for array, _, _ in items]
    full = [(lax.axis_size(axis),) + array.shape for array, axis, _ in items]
    kept = [array.shape if reduce else shape for (array, _, reduce), shape in zip(items, full)]
    sems = [pltpu.SemaphoreType.DMA((shape[0] - 1,)) for shape in full]
    return pl.pallas_call(
        functools.partial(swap_kernel, plan),
        out_shape=[jax.ShapeDtypeStruct(shape, jnp.float32) for shape in kept],
        in_specs=[pl.BlockSpec(memory_space=pltpu.VMEM)] * len(items),
        out_specs=[pl.BlockSpec(memory_space=pltpu.VMEM)] * len(items),
        scratch_shapes=[pltpu.VMEM(shape, jnp.float32) for shape in full] + sems + sems,
        compiler_params=pltpu.CompilerParams(collective_id=number, has_side_effects=True),
        name=name,
    )(*arrays)


def end_parts(normed, b_rows, dt_rows, decay_rate):
    steps_total = normed.shape[0]
    head_count = decay_rate.shape[0]
    step_size = jax.nn.softplus(dt_rows)
    running = jnp.cumsum(-step_size * decay_rate[None, :], axis=0)
    tail_weight = jnp.exp(running[-1][None, :] - running) * step_size
    head_rows = normed.reshape(steps_total, head_count, -1)
    local_state = jnp.einsum("sh,shp,sn->hpn", tail_weight, head_rows, b_rows, precision=HIGHEST)
    return (jnp.exp(running[-1]), local_state.reshape(head_count, -1))


def ssd_piece(normed, b_rows, c_rows, dt_rows, decay_rate, skip_gain, state_start):
    steps_total = normed.shape[0]
    head_count = decay_rate.shape[0]
    state_width = b_rows.shape[1]
    step_size = jax.nn.softplus(dt_rows)
    running = jnp.cumsum(-step_size * decay_rate[None, :], axis=0)
    positions = jnp.arange(steps_total, dtype=jnp.int32)
    causal = (positions[:, None] >= positions[None, :])[:, :, None]
    spread = jnp.where(causal, running[:, None, :] - running[None, :, :], 0.0)
    decay_table = jnp.where(causal, jnp.exp(spread), 0.0)
    pairing = jnp.dot(c_rows, b_rows.T, precision=HIGHEST)
    mixing = decay_table * pairing[:, :, None] * step_size[None, :, :]
    head_rows = normed.reshape(steps_total, head_count, -1)
    state_three = state_start.reshape(head_count, -1, state_width)
    mixed = jnp.einsum("tsh,shp->thp", mixing, head_rows, precision=HIGHEST)
    mixed = mixed + jnp.einsum(
        "tn,th,hpn->thp", c_rows, jnp.exp(running), state_three, precision=HIGHEST
    )
    mixed = mixed + skip_gain[None, :, None] * head_rows
    decay_total, local_state = end_parts(normed, b_rows, dt_rows, decay_rate)
    state_end = decay_total[:, None] * state_start + local_state
    return (mixed.reshape(steps_total, -1), state_end)


def carry_in(decays, states, reverse):
    peers, place = (lax.axis_size("expert"), lax.axis_index("expert"))
    held = jnp.zeros_like(states[0])
    for k in range(peers):
        at = peers - 1 - k if reverse else k
        reached = at > place if reverse else at < place
        held = jnp.where(reached, decays[at][:, None] * held + states[at], held)
    return held


def slices(total, width):
    return [(at, min(width, total - at)) for at in range(0, total, width)]


def expert_kernel(
    cap,
    send_rows,
    send_grads,
    gate_hbm,
    up_hbm,
    down_hbm,
    back_f,
    back_b,
    rows,
    grads,
    hidden,
    gate_back,
    up_back,
    gate_w,
    up_w,
    down_w,
    gate_s,
    up_s,
    away,
    mine,
    pair,
    chips,
    summed,
    z_send,
    z_recv,
    c_send,
    c_recv,
    p_send,
    p_recv,
    pair_send,
    pair_recv,
    chip_send,
    chip_recv,
    back_send,
    back_recv,
    local_sem,
    weight_sem,
):
    peers, place = (lax.axis_size("dp"), lax.axis_index("dp"))
    blocks, block = (lax.axis_size("expert"), lax.axis_index("expert"))
    chip_count = peers // 2
    chip, core = (place // 2, lax.rem(place, 2))
    partner = place + 1 - 2 * core
    width = send_rows.shape[1]
    units = gate_w.shape[1]
    sources = (send_rows, send_grads)
    wholes = (rows, grads)
    backs = (back_f, back_b)

    def strip(j):
        return pl.ds(pl.multiple_of(j * cap, 16), cap)

    def columns(d):
        return pl.ds(pl.multiple_of(d * width, 128), width)

    def ahead(k):
        return lax.rem(block + k, blocks)

    def chip_at(q):
        return lax.rem(chip + q, chip_count)

    weights = [
        pltpu.make_async_copy(hbm.at[0], held, weight_sem.at[n])
        for n, (hbm, held) in enumerate(
            ((gate_hbm, gate_w), (up_hbm, up_w), (down_hbm, down_w))
        )
    ]
    for item in weights:
        item.start()
    greet(("dp", "expert"))

    def own_copy(t):
        return pltpu.make_async_copy(
            sources[t].at[strip(block), :], wholes[t].at[strip(block), columns(place)], local_sem.at[t]
        )

    def z_copy(t, k, land):
        return pltpu.make_async_remote_copy(
            src_ref=sources[t].at[strip(ahead(k)), :],
            dst_ref=wholes[t].at[strip(land), columns(place)],
            send_sem=z_send.at[t, k],
            recv_sem=z_recv.at[t, k],
            device_id={"expert": ahead(k)},
            device_id_type=MESH,
        )

    def spread_copy(t, k, j, q, owner):
        cut = wholes[t].at[strip(j), columns(owner)]
        return pltpu.make_async_remote_copy(
            src_ref=cut,
            dst_ref=cut,
            send_sem=c_send.at[t, k * chip_count + q],
            recv_sem=c_recv.at[t, k * chip_count + q],
            device_id={"dp": 2 * chip_at(q) + core},
            device_id_type=MESH,
        )

    def partner_copy(t, k, j, q, owner):
        cut = wholes[t].at[strip(j), columns(owner)]
        return pltpu.make_async_remote_copy(
            src_ref=cut,
            dst_ref=cut,
            send_sem=p_send.at[t, k * chip_count + q],
            recv_sem=p_recv.at[t, k * chip_count + q],
            device_id={"dp": partner},
            device_id_type=MESH,
        )

    for t in range(2):
        own_copy(t).start()
        loop(blocks - 1, lambda k: z_copy(t, k + 1, block).start())

    def forward(t, k, j):
        loop(chip_count - 1, lambda q: spread_copy(t, k, j, q + 1, place).start())
        partner_copy(t, k, j, 0, place).start()

    for t in range(2):
        own_copy(t).wait()
        forward(t, 0, block)

        def pass_on(n):
            k = n + 1
            origin = lax.rem(block + blocks - k, blocks)
            z_copy(t, k, origin).wait_recv()
            forward(t, k, origin)

        loop(blocks - 1, pass_on)

    def origin_of(k):
        return lax.rem(block + blocks - k, blocks)

    def relay(t):
        def one(n):
            k, q = (n // (chip_count - 1), lax.rem(n, chip_count - 1) + 1)
            owner = 2 * lax.rem(chip + chip_count - q, chip_count) + core
            spread_copy(t, k, origin_of(k), q, owner).wait_recv()
            partner_copy(t, k, origin_of(k), q, owner).start()

        loop(blocks * (chip_count - 1), one)

        def last(n):
            k, q = (n // chip_count, lax.rem(n, chip_count))
            owner = 2 * lax.rem(chip + chip_count - q, chip_count) + 1 - core
            partner_copy(t, k, origin_of(k), q, owner).wait_recv()

        loop(blocks * chip_count, last)

    def pair_copy(t, c):
        return pltpu.make_async_remote_copy(
            src_ref=away.at[t, c],
            dst_ref=pair.at[t, c],
            send_sem=pair_send.at[t, c],
            recv_sem=pair_recv.at[t, c],
            device_id={"dp": partner},
            device_id_type=MESH,
        )

    def chip_copy(t, q):
        return pltpu.make_async_remote_copy(
            src_ref=mine.at[t, chip_at(q)],
            dst_ref=chips.at[t, q],
            send_sem=chip_send.at[t, q],
            recv_sem=chip_recv.at[t, q],
            device_id={"dp": 2 * chip_at(q) + core},
            device_id_type=MESH,
        )

    def back_copy(t, k, land):
        return pltpu.make_async_remote_copy(
            src_ref=summed.at[t, strip(ahead(k)), :],
            dst_ref=backs[t].at[strip(land), :],
            send_sem=back_send.at[t, k],
            recv_sem=back_recv.at[t, k],
            device_id={"expert": ahead(k)},
            device_id_type=MESH,
        )

    def tiles(t, term):
        def for_partner(q):
            c = chip_at(lax.rem(q + 1, chip_count))
            away[t, c] = term(2 * c + 1 - core).astype(jnp.bfloat16)
            pair_copy(t, c).start()

        loop(chip_count, for_partner)

        def for_mine(q):
            c = chip_at(lax.rem(q + 1, chip_count))
            value = term(2 * c + core)
            pair_copy(t, c).wait_recv()
            mine[t, c] = (value + pair[t, c].astype(jnp.float32)).astype(jnp.bfloat16)

            @pl.when(q < chip_count - 1)
            def _():
                chip_copy(t, q + 1).start()

        loop(chip_count, for_mine)

    def finish(t):
        total = mine[t, chip].astype(jnp.float32)
        for q in range(1, chip_count):
            chip_copy(t, q).wait_recv()
            total = total + chips[t, q].astype(jnp.float32)
        summed[t] = total.astype(jnp.bfloat16)
        loop(blocks - 1, lambda k: back_copy(t, k + 1, block).start())
        backs[t][strip(block), :] = summed[t, strip(block), :]

    relay(0)
    weights[0].wait()
    weights[1].wait()
    for at, span in slices(units, 256):
        cut = slice(at, at + span)
        gate = jnp.dot(rows[...], gate_w[:, cut], preferred_element_type=jnp.float32)
        up = jnp.dot(rows[...], up_w[:, cut], preferred_element_type=jnp.float32)
        gate_s[:, cut] = gate
        up_s[:, cut] = up
        hidden[:, cut] = (gate * jax.nn.sigmoid(gate) * up).astype(jnp.bfloat16)
    weights[2].wait()
    tiles(
        0,
        lambda d: jnp.dot(hidden[...], down_w[:, columns(d)], preferred_element_type=jnp.float32),
    )
    relay(1)
    nt = (((1,), (1,)), ((), ()))
    for at, span in slices(units, 256):
        cut = slice(at, at + span)
        unit_grad = lax.dot_general(
            grads[...], down_w[cut, :], nt, preferred_element_type=jnp.float32
        )
        gate = gate_s[:, cut]
        sigma = jax.nn.sigmoid(gate)
        gate_back[:, cut] = (
            unit_grad * up_s[:, cut] * sigma * (1.0 + gate * (1.0 - sigma))
        ).astype(jnp.bfloat16)
        up_back[:, cut] = (unit_grad * gate * sigma).astype(jnp.bfloat16)

    def input_term(d):
        at = pl.ds(pl.multiple_of(d * width, 128), width)
        first = lax.dot_general(
            gate_back[...], gate_w[at, :], nt, preferred_element_type=jnp.float32
        )
        return first + lax.dot_general(
            up_back[...], up_w[at, :], nt, preferred_element_type=jnp.float32
        )

    tiles(1, input_term)
    finish(0)
    finish(1)
    for t in range(2):

        def sent_back(n):
            copy = back_copy(t, n + 1, origin_of(n + 1))
            copy.wait_recv()
            copy.wait_send()
            z_copy(t, n + 1, block).wait_send()

        loop(blocks - 1, sent_back)
        loop(chip_count, lambda c: pair_copy(t, c).wait_send())
        loop(chip_count - 1, lambda q: chip_copy(t, q + 1).wait_send())

        def spread_done(n):
            k, q = (n // (chip_count - 1), lax.rem(n, chip_count - 1) + 1)
            spread_copy(t, k, origin_of(k), q, place).wait_send()

        loop(blocks * (chip_count - 1), spread_done)

        def partner_done(n):
            k, q = (n // chip_count, lax.rem(n, chip_count))
            partner_copy(t, k, origin_of(k), q, place).wait_send()

        loop(blocks * chip_count, partner_done)


def experts(cap, send_rows, send_grads, gate_weight, up_weight, down_weight):
    peers, blocks = (lax.axis_size("dp"), lax.axis_size("expert"))
    chip_count = peers // 2
    total, width = send_rows.shape
    features, units = gate_weight.shape[1:]
    half, full = (jnp.bfloat16, jnp.float32)
    vmem = pl.BlockSpec(memory_space=pltpu.VMEM)
    hbm = pl.BlockSpec(memory_space=pl.ANY)
    dma = pltpu.SemaphoreType.DMA
    shapes = [(total, width)] * 2 + [(total, features)] * 2 + [(total, units)] * 3
    return pl.pallas_call(
        functools.partial(expert_kernel, cap),
        out_shape=[jax.ShapeDtypeStruct(shape, half) for shape in shapes],
        in_specs=[vmem, vmem, hbm, hbm, hbm],
        out_specs=[vmem] * 7,
        scratch_shapes=[
            pltpu.VMEM((features, units), half),
            pltpu.VMEM((features, units), half),
            pltpu.VMEM((units, features), half),
            pltpu.VMEM((total, units), full),
            pltpu.VMEM((total, units), full),
            pltpu.VMEM((2, chip_count, total, width), half),
            pltpu.VMEM((2, chip_count, total, width), half),
            pltpu.VMEM((2, chip_count, total, width), half),
            pltpu.VMEM((2, chip_count, total, width), half),
            pltpu.VMEM((2, total, width), half),
            dma((2, blocks)),
            dma((2, blocks)),
            dma((2, blocks * chip_count)),
            dma((2, blocks * chip_count)),
            dma((2, blocks * chip_count)),
            dma((2, blocks * chip_count)),
            dma((2, chip_count)),
            dma((2, chip_count)),
            dma((2, chip_count)),
            dma((2, chip_count)),
            dma((2, blocks)),
            dma((2, blocks)),
            dma((2,)),
            dma((3,)),
        ],
        compiler_params=pltpu.CompilerParams(collective_id=7, has_side_effects=True),
        name="experts",
    )(send_rows, send_grads, gate_weight, up_weight, down_weight)


def body(
    tokens,
    routes,
    dt_raw,
    b_proj,
    c_proj,
    decay_rate,
    skip_gain,
    router_weight,
    gate_weight,
    up_weight,
    down_weight,
    out_grad,
):
    tok_count, width = tokens.shape
    expert_count = lax.axis_size("expert")
    features = width * lax.axis_size("dp")
    head_count = decay_rate.shape[0]
    capacity = 5 * tok_count // (2 * expert_count)
    padded = -(-capacity // 16) * 16
    inputs = tokens.astype(jnp.float32)
    (square_one,) = swap("sum_one", 1, (jnp.sum(inputs * inputs, axis=1)[None], "dp", True))
    scale_one = lax.rsqrt(square_one[0][:, None] / features + EPSILON)
    normed = inputs * scale_one
    decay_total, local_state = end_parts(normed, b_proj, dt_raw, decay_rate)
    state_width = local_state.shape[1]
    packed = jnp.concatenate(
        [local_state, jnp.broadcast_to(decay_total[:, None], (head_count, 128))], axis=1
    )
    (ends,) = swap("state_one", 2, (packed, "expert", False))
    decays = ends[:, :, state_width]
    state_in = carry_in(decays, ends[:, :, :state_width], False)

    def mixer(normed_in, rate_in, skip_in, state_start):
        return ssd_piece(normed_in, b_proj, c_proj, dt_raw, rate_in, skip_in, state_start)

    (mixed, state_end), mixer_pull = jax.vjp(mixer, normed, decay_rate, skip_gain, state_in)
    resid = (inputs + mixed).astype(jnp.bfloat16)
    resid_f = resid.astype(jnp.float32)
    raw_part = lax.dot_general(
        router_weight, resid_f, (((0,), (1,)), ((), ())), precision=HIGHEST
    )
    stats = jnp.concatenate([jnp.sum(resid_f * resid_f, axis=1)[None], raw_part], axis=0)
    (stats,) = swap("sum_two", 3, (stats, "dp", True))
    scale_row = lax.rsqrt(stats[0] / features + EPSILON)
    scale_two = scale_row[:, None]
    moe_in = (resid_f * scale_two).astype(jnp.bfloat16)
    expert_ids = jnp.arange(expert_count, dtype=jnp.int32)
    first_hot = (routes[:, 0:1] == expert_ids[None, :]).astype(jnp.float32)
    second_hot = (routes[:, 1:2] == expert_ids[None, :]).astype(jnp.float32)
    hot_gap = first_hot - second_hot
    raw_gap = jnp.sum(stats[1:].T * hot_gap, axis=1)
    logit_gap = raw_gap * scale_row
    first_weight = jax.nn.sigmoid(logit_gap)
    second_weight = jax.nn.sigmoid(-logit_gap)
    positions = jnp.arange(tok_count, dtype=jnp.int32)
    lower = (positions[:, None] > positions[None, :]).astype(jnp.bfloat16)
    both_hot = (first_hot + second_hot).astype(jnp.bfloat16)
    earlier = jnp.dot(lower, both_hot, preferred_element_type=jnp.float32)

    def slot_of(hot, ids):
        index = jnp.sum(earlier * hot, axis=1)
        target = ids.astype(jnp.float32) * padded + index
        return jnp.where(index < capacity, target, -1.0)

    slot_ids = jnp.arange(expert_count * padded, dtype=jnp.int32).astype(jnp.float32)[:, None]
    first_table = slot_ids == slot_of(first_hot, routes[:, 0])[None, :]
    second_table = slot_ids == slot_of(second_hot, routes[:, 1])[None, :]
    either = (first_table | second_table).astype(jnp.bfloat16)
    slot_weight = jnp.sum(
        jnp.where(first_table, first_weight[None, :], 0.0)
        + jnp.where(second_table, second_weight[None, :], 0.0),
        axis=1,
        keepdims=True,
    )
    send_rows = jnp.dot(either, moe_in, preferred_element_type=jnp.float32).astype(jnp.bfloat16)
    send_grads = jnp.dot(either, out_grad, preferred_element_type=jnp.float32) * slot_weight
    back_f, back_b, unit_rows, grad_rows, hidden, gate_back, up_back = experts(
        padded, send_rows, send_grads.astype(jnp.bfloat16), gate_weight, up_weight, down_weight
    )
    tn = (((0,), (0,)), ((), ()))
    down_part = lax.dot_general(hidden, grad_rows, tn, preferred_element_type=jnp.float32)
    gate_part = lax.dot_general(unit_rows, gate_back, tn, preferred_element_type=jnp.float32)
    up_part = lax.dot_general(unit_rows, up_back, tn, preferred_element_type=jnp.float32)
    pair_table = jnp.concatenate([first_table, second_table], axis=1).astype(jnp.bfloat16)
    per_slot = lax.dot_general(pair_table, back_f, tn, preferred_element_type=jnp.float32)
    first_out, second_out = (per_slot[:tok_count], per_slot[tok_count:])
    moe_sum = first_weight[:, None] * first_out + second_weight[:, None] * second_out
    block_out = (resid_f + moe_sum).astype(jnp.bfloat16)
    moe_grad = lax.dot_general(either, back_b, tn, preferred_element_type=jnp.float32)
    upstream = out_grad.astype(jnp.float32)
    inner_parts = jnp.stack(
        [
            jnp.sum(upstream * first_out, axis=1),
            jnp.sum(upstream * second_out, axis=1),
            jnp.sum(resid_f * moe_grad, axis=1),
        ]
    )
    (inner_all,) = swap("sum_three", 4, (inner_parts, "dp", True))
    gap_grad = first_weight * second_weight * (inner_all[0] - inner_all[1])
    inner = inner_all[2] + gap_grad * raw_gap
    logit_grad = gap_grad[:, None] * hot_gap
    moe_in_grad = moe_grad + jnp.dot(logit_grad, router_weight.T, precision=HIGHEST)
    router_part = lax.dot_general(logit_grad, moe_in.astype(jnp.float32), tn, precision=HIGHEST)
    resid_grad = (
        upstream
        + scale_two * moe_in_grad
        - resid_f * (scale_two * scale_two * scale_two) * (inner[:, None] / features)
    )
    running = jnp.cumsum(-jax.nn.softplus(dt_raw) * decay_rate[None, :], axis=0)
    grad_heads = resid_grad.reshape(tok_count, head_count, -1)
    state_grad = jnp.einsum(
        "th,thp,tn->hpn", jnp.exp(running), grad_heads, c_proj, precision=HIGHEST
    ).reshape(head_count, -1)
    grad_ends, router_total = swap(
        "state_two", 5, (state_grad, "expert", False), (router_part, "expert", True)
    )
    later_grad = carry_in(decays, grad_ends, True)
    normed_grad, rate_part, skip_part, _ = mixer_pull((resid_grad, later_grad))
    inner_one = jnp.sum(normed_grad * inputs, axis=1)[None]
    small = jnp.pad(jnp.stack([rate_part, skip_part]), ((0, 0), (0, 128 - head_count)))
    inner_one, small = swap("sum_four", 6, (inner_one, "dp", True), (small, "expert", True))
    token_grad = (
        resid_grad
        + scale_one * normed_grad
        - inputs * (scale_one * scale_one * scale_one) * (inner_one[0][:, None] / features)
    )
    return (
        block_out,
        token_grad.astype(jnp.bfloat16),
        gate_part.astype(jnp.bfloat16)[None],
        up_part.astype(jnp.bfloat16)[None],
        down_part.astype(jnp.bfloat16)[None],
        router_total.T,
        small[0, :head_count],
        small[1, :head_count],
    )


def solution(mesh):
    return jax.shard_map(
        body,
        mesh=mesh,
        in_specs=(
            P("expert", "dp"),
            P("expert", None),
            P("expert", "dp"),
            P("expert", None),
            P("expert", None),
            P("dp"),
            P("dp"),
            P("dp", None),
            P("expert", None, "dp"),
            P("expert", None, "dp"),
            P("expert", "dp", None),
            P("expert", "dp"),
        ),
        out_specs=(
            P("expert", "dp"),
            P("expert", "dp"),
            P("expert", None, "dp"),
            P("expert", None, "dp"),
            P("expert", "dp", None),
            P("dp", None),
            P("dp"),
            P("dp"),
        ),
        check_vma=False,
    )
```

```python
import functools
import jax
import jax.numpy as jnp
from jax import lax
from jax.experimental import pallas as pl
from jax.experimental.pallas import tpu as pltpu
from jax.sharding import PartitionSpec as P


EPSILON = 1e-06
HIGHEST = lax.Precision.HIGHEST
MESH = pl.DeviceIdType.MESH


def loop(count, step):
    def run(i, carry):
        step(i)
        return carry

    lax.fori_loop(0, count, run, 0)


def greet(axes):
    barrier = pltpu.get_barrier_semaphore()
    total = 0
    for axis in axes:
        peers, place = (lax.axis_size(axis), lax.axis_index(axis))
        total += peers - 1

        def signal(k):
            pl.semaphore_signal(
                barrier, 1, device_id={axis: lax.rem(place + k + 1, peers)}, device_id_type=MESH
            )

        loop(peers - 1, signal)
    pl.semaphore_wait(barrier, total)


def swap_kernel(plan, *refs):
    amount = len(plan)
    ins, outs = (refs[:amount], refs[amount : 2 * amount])
    gathered = refs[2 * amount : 3 * amount]
    sends, recvs = (refs[3 * amount : 4 * amount], refs[4 * amount : 5 * amount])
    greet(sorted({axis for axis, _ in plan}))

    def copy_of(item, k):
        axis = plan[item][0]
        peers, place = (lax.axis_size(axis), lax.axis_index(axis))
        return pltpu.make_async_remote_copy(
            src_ref=ins[item],
            dst_ref=gathered[item].at[place],
            send_sem=sends[item].at[k],
            recv_sem=recvs[item].at[k],
            device_id={axis: lax.rem(place + k + 1, peers)},
            device_id_type=MESH,
        )

    for item, (axis, _) in enumerate(plan):
        loop(lax.axis_size(axis) - 1, lambda k: copy_of(item, k).start())
        gathered[item][lax.axis_index(axis)] = ins[item][...]
    for item, (axis, reduce) in enumerate(plan):
        peers, place = (lax.axis_size(axis), lax.axis_index(axis))

        def arrive(k):
            pltpu.make_async_remote_copy(
                src_ref=ins[item],
                dst_ref=gathered[item].at[lax.rem(place + peers - k - 1, peers)],
                send_sem=sends[item].at[k],
                recv_sem=recvs[item].at[k],
                device_id={axis: lax.rem(place + k + 1, peers)},
                device_id_type=MESH,
            ).wait()

        loop(peers - 1, arrive)
        if reduce:
            outs[item][...] = jnp.sum(gathered[item][...], axis=0)
        else:
            outs[item][...] = gathered[item][...]


def swap(name, number, *items):
    plan = tuple((axis, reduce) for _, axis, reduce in items)
    arrays = [array for array, _, _ in items]
    full = [(lax.axis_size(axis),) + array.shape for array, axis, _ in items]
    kept = [array.shape if reduce else shape for (array, _, reduce), shape in zip(items, full)]
    sems = [pltpu.SemaphoreType.DMA((shape[0] - 1,)) for shape in full]
    return pl.pallas_call(
        functools.partial(swap_kernel, plan),
        out_shape=[jax.ShapeDtypeStruct(shape, jnp.float32) for shape in kept],
        in_specs=[pl.BlockSpec(memory_space=pltpu.VMEM)] * len(items),
        out_specs=[pl.BlockSpec(memory_space=pltpu.VMEM)] * len(items),
        scratch_shapes=[pltpu.VMEM(shape, jnp.float32) for shape in full] + sems + sems,
        compiler_params=pltpu.CompilerParams(collective_id=number, has_side_effects=True),
        name=name,
    )(*arrays)


def running_sum(values):
    positions = jnp.arange(values.shape[0], dtype=jnp.int32)
    reached = (positions[:, None] >= positions[None, :]).astype(jnp.float32)
    return jnp.dot(reached, values, precision=HIGHEST)


def end_parts(normed, b_rows, dt_rows, decay_rate):
    steps_total = normed.shape[0]
    head_count = decay_rate.shape[0]
    step_size = jax.nn.softplus(dt_rows)
    running = running_sum(-step_size * decay_rate[None, :])
    tail_weight = jnp.exp(running[-1][None, :] - running) * step_size
    head_rows = normed.reshape(steps_total, head_count, -1)
    local_state = jnp.einsum("sh,shp,sn->hpn", tail_weight, head_rows, b_rows, precision=HIGHEST)
    return (jnp.exp(running[-1]), local_state.reshape(head_count, -1))


def ssd_piece(normed, b_rows, c_rows, dt_rows, decay_rate, skip_gain, state_start):
    steps_total = normed.shape[0]
    head_count = decay_rate.shape[0]
    state_width = b_rows.shape[1]
    step_size = jax.nn.softplus(dt_rows)
    running = running_sum(-step_size * decay_rate[None, :])
    positions = jnp.arange(steps_total, dtype=jnp.int32)
    causal = (positions[:, None] >= positions[None, :])[:, :, None]
    spread = jnp.where(causal, running[:, None, :] - running[None, :, :], 0.0)
    decay_table = jnp.where(causal, jnp.exp(spread), 0.0)
    pairing = jnp.dot(c_rows, b_rows.T, precision=HIGHEST)
    mixing = decay_table * pairing[:, :, None] * step_size[None, :, :]
    head_rows = normed.reshape(steps_total, head_count, -1)
    state_three = state_start.reshape(head_count, -1, state_width)
    mixed = jnp.einsum("tsh,shp->thp", mixing, head_rows, precision=HIGHEST)
    mixed = mixed + jnp.einsum(
        "tn,th,hpn->thp", c_rows, jnp.exp(running), state_three, precision=HIGHEST
    )
    mixed = mixed + skip_gain[None, :, None] * head_rows
    decay_total, local_state = end_parts(normed, b_rows, dt_rows, decay_rate)
    state_end = decay_total[:, None] * state_start + local_state
    return (mixed.reshape(steps_total, -1), state_end)


def carry_in(decays, states, reverse):
    peers, place = (lax.axis_size("expert"), lax.axis_index("expert"))
    held = jnp.zeros_like(states[0])
    for k in range(peers):
        at = peers - 1 - k if reverse else k
        reached = at > place if reverse else at < place
        held = jnp.where(reached, decays[at][:, None] * held + states[at], held)
    return held


def slices(total, width):
    return [(at, min(width, total - at)) for at in range(0, total, width)]


def expert_kernel(
    cap,
    send_rows,
    send_grads,
    gate_hbm,
    up_hbm,
    down_hbm,
    back_f,
    back_b,
    rows,
    grads,
    hidden,
    gate_back,
    up_back,
    gate_w,
    up_w,
    down_w,
    gate_s,
    up_s,
    away,
    mine,
    pair,
    chips,
    summed,
    z_send,
    z_recv,
    c_send,
    c_recv,
    p_send,
    p_recv,
    pair_send,
    pair_recv,
    chip_send,
    chip_recv,
    back_send,
    back_recv,
    local_sem,
    weight_sem,
):
    peers, place = (lax.axis_size("dp"), lax.axis_index("dp"))
    blocks, block = (lax.axis_size("expert"), lax.axis_index("expert"))
    chip_count = peers // 2
    chip, core = (place // 2, lax.rem(place, 2))
    partner = place + 1 - 2 * core
    width = send_rows.shape[1]
    units = gate_w.shape[1]
    sources = (send_rows, send_grads)
    wholes = (rows, grads)
    backs = (back_f, back_b)

    def strip(j):
        return pl.ds(pl.multiple_of(j * cap, 16), cap)

    def columns(d):
        return pl.ds(pl.multiple_of(d * width, 128), width)

    def ahead(k):
        return lax.rem(block + k, blocks)

    def chip_at(q):
        return lax.rem(chip + q, chip_count)

    weights = [
        pltpu.make_async_copy(hbm.at[0], held, weight_sem.at[n])
        for n, (hbm, held) in enumerate(
            ((gate_hbm, gate_w), (up_hbm, up_w), (down_hbm, down_w))
        )
    ]
    for item in weights:
        item.start()
    greet(("dp", "expert"))

    def own_copy(t):
        return pltpu.make_async_copy(
            sources[t].at[strip(block), :], wholes[t].at[strip(block), columns(place)], local_sem.at[t]
        )

    def z_copy(t, k, land):
        return pltpu.make_async_remote_copy(
            src_ref=sources[t].at[strip(ahead(k)), :],
            dst_ref=wholes[t].at[strip(land), columns(place)],
            send_sem=z_send.at[t, k],
            recv_sem=z_recv.at[t, k],
            device_id={"expert": ahead(k)},
            device_id_type=MESH,
        )

    def spread_copy(t, k, j, q, owner):
        cut = wholes[t].at[strip(j), columns(owner)]
        return pltpu.make_async_remote_copy(
            src_ref=cut,
            dst_ref=cut,
            send_sem=c_send.at[t, k * chip_count + q],
            recv_sem=c_recv.at[t, k * chip_count + q],
            device_id={"dp": 2 * chip_at(q) + core},
            device_id_type=MESH,
        )

    def partner_copy(t, k, j, q, owner):
        cut = wholes[t].at[strip(j), columns(owner)]
        return pltpu.make_async_remote_copy(
            src_ref=cut,
            dst_ref=cut,
            send_sem=p_send.at[t, k * chip_count + q],
            recv_sem=p_recv.at[t, k * chip_count + q],
            device_id={"dp": partner},
            device_id_type=MESH,
        )

    for t in range(2):
        own_copy(t).start()
        loop(blocks - 1, lambda k: z_copy(t, k + 1, block).start())

    def forward(t, k, j):
        loop(chip_count - 1, lambda q: spread_copy(t, k, j, q + 1, place).start())
        partner_copy(t, k, j, 0, place).start()

    for t in range(2):
        own_copy(t).wait()
        forward(t, 0, block)

        def pass_on(n):
            k = n + 1
            origin = lax.rem(block + blocks - k, blocks)
            z_copy(t, k, origin).wait_recv()
            forward(t, k, origin)

        loop(blocks - 1, pass_on)

    def origin_of(k):
        return lax.rem(block + blocks - k, blocks)

    def relay(t):
        def one(n):
            k, q = (n // (chip_count - 1), lax.rem(n, chip_count - 1) + 1)
            owner = 2 * lax.rem(chip + chip_count - q, chip_count) + core
            spread_copy(t, k, origin_of(k), q, owner).wait_recv()
            partner_copy(t, k, origin_of(k), q, owner).start()

        loop(blocks * (chip_count - 1), one)

        def last(n):
            k, q = (n // chip_count, lax.rem(n, chip_count))
            owner = 2 * lax.rem(chip + chip_count - q, chip_count) + 1 - core
            partner_copy(t, k, origin_of(k), q, owner).wait_recv()

        loop(blocks * chip_count, last)

    def pair_copy(t, c):
        return pltpu.make_async_remote_copy(
            src_ref=away.at[t, c],
            dst_ref=pair.at[t, c],
            send_sem=pair_send.at[t, c],
            recv_sem=pair_recv.at[t, c],
            device_id={"dp": partner},
            device_id_type=MESH,
        )

    def chip_copy(t, q):
        return pltpu.make_async_remote_copy(
            src_ref=mine.at[t, chip_at(q)],
            dst_ref=chips.at[t, q],
            send_sem=chip_send.at[t, q],
            recv_sem=chip_recv.at[t, q],
            device_id={"dp": 2 * chip_at(q) + core},
            device_id_type=MESH,
        )

    def back_copy(t, k, land):
        return pltpu.make_async_remote_copy(
            src_ref=summed.at[t, strip(ahead(k)), :],
            dst_ref=backs[t].at[strip(land), :],
            send_sem=back_send.at[t, k],
            recv_sem=back_recv.at[t, k],
            device_id={"expert": ahead(k)},
            device_id_type=MESH,
        )

    def tiles(t, term):
        def for_partner(q):
            c = chip_at(lax.rem(q + 1, chip_count))
            away[t, c] = term(2 * c + 1 - core).astype(jnp.bfloat16)
            pair_copy(t, c).start()

        loop(chip_count, for_partner)

        def for_mine(q):
            c = chip_at(lax.rem(q + 1, chip_count))
            value = term(2 * c + core)
            pair_copy(t, c).wait_recv()
            mine[t, c] = (value + pair[t, c].astype(jnp.float32)).astype(jnp.bfloat16)

            @pl.when(q < chip_count - 1)
            def _():
                chip_copy(t, q + 1).start()

        loop(chip_count, for_mine)

    def finish(t):
        total = mine[t, chip].astype(jnp.float32)
        for q in range(1, chip_count):
            chip_copy(t, q).wait_recv()
            total = total + chips[t, q].astype(jnp.float32)
        summed[t] = total.astype(jnp.bfloat16)
        loop(blocks - 1, lambda k: back_copy(t, k + 1, block).start())
        backs[t][strip(block), :] = summed[t, strip(block), :]

    relay(0)
    weights[0].wait()
    weights[1].wait()
    for at, span in slices(units, 256):
        cut = slice(at, at + span)
        gate = jnp.dot(rows[...], gate_w[:, cut], preferred_element_type=jnp.float32)
        up = jnp.dot(rows[...], up_w[:, cut], preferred_element_type=jnp.float32)
        gate_s[:, cut] = gate
        up_s[:, cut] = up
        hidden[:, cut] = (gate * jax.nn.sigmoid(gate) * up).astype(jnp.bfloat16)
    weights[2].wait()
    tiles(
        0,
        lambda d: jnp.dot(hidden[...], down_w[:, columns(d)], preferred_element_type=jnp.float32),
    )
    relay(1)
    nt = (((1,), (1,)), ((), ()))
    for at, span in slices(units, 256):
        cut = slice(at, at + span)
        unit_grad = lax.dot_general(
            grads[...], down_w[cut, :], nt, preferred_element_type=jnp.float32
        )
        gate = gate_s[:, cut]
        sigma = jax.nn.sigmoid(gate)
        gate_back[:, cut] = (
            unit_grad * up_s[:, cut] * sigma * (1.0 + gate * (1.0 - sigma))
        ).astype(jnp.bfloat16)
        up_back[:, cut] = (unit_grad * gate * sigma).astype(jnp.bfloat16)

    def input_term(d):
        at = pl.ds(pl.multiple_of(d * width, 128), width)
        first = lax.dot_general(
            gate_back[...], gate_w[at, :], nt, preferred_element_type=jnp.float32
        )
        return first + lax.dot_general(
            up_back[...], up_w[at, :], nt, preferred_element_type=jnp.float32
        )

    tiles(1, input_term)
    finish(0)
    finish(1)
    for t in range(2):

        def sent_back(n):
            copy = back_copy(t, n + 1, origin_of(n + 1))
            copy.wait_recv()
            copy.wait_send()
            z_copy(t, n + 1, block).wait_send()

        loop(blocks - 1, sent_back)
        loop(chip_count, lambda c: pair_copy(t, c).wait_send())
        loop(chip_count - 1, lambda q: chip_copy(t, q + 1).wait_send())

        def spread_done(n):
            k, q = (n // (chip_count - 1), lax.rem(n, chip_count - 1) + 1)
            spread_copy(t, k, origin_of(k), q, place).wait_send()

        loop(blocks * (chip_count - 1), spread_done)

        def partner_done(n):
            k, q = (n // chip_count, lax.rem(n, chip_count))
            partner_copy(t, k, origin_of(k), q, place).wait_send()

        loop(blocks * chip_count, partner_done)


def experts(cap, send_rows, send_grads, gate_weight, up_weight, down_weight):
    peers, blocks = (lax.axis_size("dp"), lax.axis_size("expert"))
    chip_count = peers // 2
    total, width = send_rows.shape
    features, units = gate_weight.shape[1:]
    half, full = (jnp.bfloat16, jnp.float32)
    vmem = pl.BlockSpec(memory_space=pltpu.VMEM)
    hbm = pl.BlockSpec(memory_space=pl.ANY)
    dma = pltpu.SemaphoreType.DMA
    shapes = [(total, width)] * 2 + [(total, features)] * 2 + [(total, units)] * 3
    return pl.pallas_call(
        functools.partial(expert_kernel, cap),
        out_shape=[jax.ShapeDtypeStruct(shape, half) for shape in shapes],
        in_specs=[vmem, vmem, hbm, hbm, hbm],
        out_specs=[vmem] * 7,
        scratch_shapes=[
            pltpu.VMEM((features, units), half),
            pltpu.VMEM((features, units), half),
            pltpu.VMEM((units, features), half),
            pltpu.VMEM((total, units), full),
            pltpu.VMEM((total, units), full),
            pltpu.VMEM((2, chip_count, total, width), half),
            pltpu.VMEM((2, chip_count, total, width), half),
            pltpu.VMEM((2, chip_count, total, width), half),
            pltpu.VMEM((2, chip_count, total, width), half),
            pltpu.VMEM((2, total, width), half),
            dma((2, blocks)),
            dma((2, blocks)),
            dma((2, blocks * chip_count)),
            dma((2, blocks * chip_count)),
            dma((2, blocks * chip_count)),
            dma((2, blocks * chip_count)),
            dma((2, chip_count)),
            dma((2, chip_count)),
            dma((2, chip_count)),
            dma((2, chip_count)),
            dma((2, blocks)),
            dma((2, blocks)),
            dma((2,)),
            dma((3,)),
        ],
        compiler_params=pltpu.CompilerParams(collective_id=7, has_side_effects=True),
        name="experts",
    )(send_rows, send_grads, gate_weight, up_weight, down_weight)


def body(
    tokens,
    routes,
    dt_raw,
    b_proj,
    c_proj,
    decay_rate,
    skip_gain,
    router_weight,
    gate_weight,
    up_weight,
    down_weight,
    out_grad,
):
    tok_count, width = tokens.shape
    expert_count = lax.axis_size("expert")
    features = width * lax.axis_size("dp")
    head_count = decay_rate.shape[0]
    capacity = 5 * tok_count // (2 * expert_count)
    padded = -(-capacity // 16) * 16
    inputs = tokens.astype(jnp.float32)
    (square_one,) = swap("sum_one", 1, (jnp.sum(inputs * inputs, axis=1)[None], "dp", True))
    scale_one = lax.rsqrt(square_one[0][:, None] / features + EPSILON)
    normed = inputs * scale_one
    decay_total, local_state = end_parts(normed, b_proj, dt_raw, decay_rate)
    state_width = local_state.shape[1]
    packed = jnp.concatenate(
        [local_state, jnp.broadcast_to(decay_total[:, None], (head_count, 128))], axis=1
    )
    (ends,) = swap("state_one", 2, (packed, "expert", False))
    decays = ends[:, :, state_width]
    state_in = carry_in(decays, ends[:, :, :state_width], False)

    def mixer(normed_in, rate_in, skip_in, state_start):
        return ssd_piece(normed_in, b_proj, c_proj, dt_raw, rate_in, skip_in, state_start)

    (mixed, state_end), mixer_pull = jax.vjp(mixer, normed, decay_rate, skip_gain, state_in)
    resid = (inputs + mixed).astype(jnp.bfloat16)
    resid_f = resid.astype(jnp.float32)
    raw_part = lax.dot_general(
        router_weight, resid_f, (((0,), (1,)), ((), ())), precision=HIGHEST
    )
    stats = jnp.concatenate([jnp.sum(resid_f * resid_f, axis=1)[None], raw_part], axis=0)
    (stats,) = swap("sum_two", 3, (stats, "dp", True))
    scale_row = lax.rsqrt(stats[0] / features + EPSILON)
    scale_two = scale_row[:, None]
    moe_in = (resid_f * scale_two).astype(jnp.bfloat16)
    expert_ids = jnp.arange(expert_count, dtype=jnp.int32)
    first_hot = (routes[:, 0:1] == expert_ids[None, :]).astype(jnp.float32)
    second_hot = (routes[:, 1:2] == expert_ids[None, :]).astype(jnp.float32)
    hot_gap = first_hot - second_hot
    raw_gap = jnp.sum(stats[1:].T * hot_gap, axis=1)
    logit_gap = raw_gap * scale_row
    first_weight = jax.nn.sigmoid(logit_gap)
    second_weight = jax.nn.sigmoid(-logit_gap)
    positions = jnp.arange(tok_count, dtype=jnp.int32)
    lower = (positions[:, None] > positions[None, :]).astype(jnp.bfloat16)
    both_hot = (first_hot + second_hot).astype(jnp.bfloat16)
    earlier = jnp.dot(lower, both_hot, preferred_element_type=jnp.float32)

    def slot_of(hot, ids):
        index = jnp.sum(earlier * hot, axis=1)
        target = ids.astype(jnp.float32) * padded + index
        return jnp.where(index < capacity, target, -1.0)

    slot_ids = jnp.arange(expert_count * padded, dtype=jnp.int32).astype(jnp.float32)[:, None]
    first_table = slot_ids == slot_of(first_hot, routes[:, 0])[None, :]
    second_table = slot_ids == slot_of(second_hot, routes[:, 1])[None, :]
    either = (first_table | second_table).astype(jnp.bfloat16)
    slot_weight = jnp.sum(
        jnp.where(first_table, first_weight[None, :], 0.0)
        + jnp.where(second_table, second_weight[None, :], 0.0),
        axis=1,
        keepdims=True,
    )
    send_rows = jnp.dot(either, moe_in, preferred_element_type=jnp.float32).astype(jnp.bfloat16)
    send_grads = jnp.dot(either, out_grad, preferred_element_type=jnp.float32) * slot_weight
    back_f, back_b, unit_rows, grad_rows, hidden, gate_back, up_back = experts(
        padded, send_rows, send_grads.astype(jnp.bfloat16), gate_weight, up_weight, down_weight
    )
    tn = (((0,), (0,)), ((), ()))
    down_part = lax.dot_general(hidden, grad_rows, tn, preferred_element_type=jnp.float32)
    gate_part = lax.dot_general(unit_rows, gate_back, tn, preferred_element_type=jnp.float32)
    up_part = lax.dot_general(unit_rows, up_back, tn, preferred_element_type=jnp.float32)
    pair_table = jnp.concatenate([first_table, second_table], axis=1).astype(jnp.bfloat16)
    per_slot = lax.dot_general(pair_table, back_f, tn, preferred_element_type=jnp.float32)
    first_out, second_out = (per_slot[:tok_count], per_slot[tok_count:])
    moe_sum = first_weight[:, None] * first_out + second_weight[:, None] * second_out
    block_out = (resid_f + moe_sum).astype(jnp.bfloat16)
    moe_grad = lax.dot_general(either, back_b, tn, preferred_element_type=jnp.float32)
    upstream = out_grad.astype(jnp.float32)
    inner_parts = jnp.stack(
        [
            jnp.sum(upstream * first_out, axis=1),
            jnp.sum(upstream * second_out, axis=1),
            jnp.sum(resid_f * moe_grad, axis=1),
        ]
    )
    (inner_all,) = swap("sum_three", 4, (inner_parts, "dp", True))
    gap_grad = first_weight * second_weight * (inner_all[0] - inner_all[1])
    inner = inner_all[2] + gap_grad * raw_gap
    logit_grad = gap_grad[:, None] * hot_gap
    moe_in_grad = moe_grad + jnp.dot(logit_grad, router_weight.T, precision=HIGHEST)
    router_part = lax.dot_general(logit_grad, moe_in.astype(jnp.float32), tn, precision=HIGHEST)
    resid_grad = (
        upstream
        + scale_two * moe_in_grad
        - resid_f * (scale_two * scale_two * scale_two) * (inner[:, None] / features)
    )
    running = running_sum(-jax.nn.softplus(dt_raw) * decay_rate[None, :])
    grad_heads = resid_grad.reshape(tok_count, head_count, -1)
    state_grad = jnp.einsum(
        "th,thp,tn->hpn", jnp.exp(running), grad_heads, c_proj, precision=HIGHEST
    ).reshape(head_count, -1)
    grad_ends, router_total = swap(
        "state_two", 5, (state_grad, "expert", False), (router_part, "expert", True)
    )
    later_grad = carry_in(decays, grad_ends, True)
    normed_grad, rate_part, skip_part, _ = mixer_pull((resid_grad, later_grad))
    inner_one = jnp.sum(normed_grad * inputs, axis=1)[None]
    small = jnp.pad(jnp.stack([rate_part, skip_part]), ((0, 0), (0, 128 - head_count)))
    inner_one, small = swap("sum_four", 6, (inner_one, "dp", True), (small, "expert", True))
    token_grad = (
        resid_grad
        + scale_one * normed_grad
        - inputs * (scale_one * scale_one * scale_one) * (inner_one[0][:, None] / features)
    )
    return (
        block_out,
        token_grad.astype(jnp.bfloat16),
        gate_part.astype(jnp.bfloat16)[None],
        up_part.astype(jnp.bfloat16)[None],
        down_part.astype(jnp.bfloat16)[None],
        router_total.T,
        small[0, :head_count],
        small[1, :head_count],
    )


def solution(mesh):
    return jax.shard_map(
        body,
        mesh=mesh,
        in_specs=(
            P("expert", "dp"),
            P("expert", None),
            P("expert", "dp"),
            P("expert", None),
            P("expert", None),
            P("dp"),
            P("dp"),
            P("dp", None),
            P("expert", None, "dp"),
            P("expert", None, "dp"),
            P("expert", "dp", None),
            P("expert", "dp"),
        ),
        out_specs=(
            P("expert", "dp"),
            P("expert", "dp"),
            P("expert", None, "dp"),
            P("expert", None, "dp"),
            P("expert", "dp", None),
            P("dp", None),
            P("dp"),
            P("dp"),
        ),
        check_vma=False,
    )
```
